32 devices in a mesh: segment: 4 (over y, core), shard: 8 (over z, x).
Axes of the slice: x: 2, y: 2, z: 4, core: 2. Of those that a mesh axis runs over, the one named last changes fastest.
Arguments:
- buffer: bfloat16 [8, 18432, 2304], P('segment', 'shard'), may hold values from -6 to 6
- right_basis: bfloat16 [8, 2304, 256], P('segment', 'shard'), may hold values from -0.125 to 0.125
- layer_count: int32 [4], P('segment'), may hold values from 1 to 2, as said below
Outputs:
- momentum_out: bfloat16 [8, 18432, 2304], P('segment', 'shard')
- left_step: bfloat16 [8, 18432, 256], P('segment', 'shard')
- right_step: float32 [8, 2304, 256], P('segment', 'shard')
The draws below stay inside these ranges and needn't reach their ends.
Inputs may be any that keep to these rules, and one draw needn't show every extreme that they name: `layer_count`: each segment uses between 1 and 2 slots; some segment uses 2 and some segment uses 1.
All inputs are finite; a program needn't handle non-finite values.
Results may differ from the reference program's by a relative error of at most 0.0024.
Values may be sent and summed in bfloat16 or wider, within the bound.
A program may use at most 128 MiB of HBM per device.

```python
import math
import jax
import jax.numpy as jnp
from jax import lax

ROWS = 18432
COLS = 2304
RANK = 256
SLOTS = 2
LAYER_SLOTS = 8
N_SEGMENT = 4
N_SHARD = 8


def draw_buffer(key, part):
    base = jax.random.fold_in(key, 11)
    first, second = jax.random.split(base, 2)
    rows_dev = ROWS // N_SHARD
    noise = jnp.clip(jax.random.normal(first, (LAYER_SLOTS, N_SHARD, rows_dev, COLS), jnp.float32), -4.0, 4.0)
    logs = jax.random.uniform(second, (LAYER_SLOTS, N_SHARD, 1, 1), jnp.float32, math.log(0.03), math.log(1.0))
    values = jnp.clip(noise * jnp.exp(logs), -6.0, 6.0)
    return values.reshape(LAYER_SLOTS, ROWS, COLS).astype(jnp.bfloat16)


def draw_layer_count(key, part):
    base = jax.random.fold_in(key, 23)
    first, second, third = jax.random.split(base, 3)
    counts = jax.random.randint(first, (N_SEGMENT,), 1, SLOTS + 1)
    fullest = jax.random.randint(second, (), 0, N_SEGMENT)
    lightest = (fullest + 1 + jax.random.randint(third, (), 0, N_SEGMENT - 1)) % N_SEGMENT
    counts = counts.at[fullest].set(SLOTS)
    counts = counts.at[lightest].set(1)
    return counts.astype(jnp.int32)


def shard_levels(rng, shape, pieces, smallest, high):
    def one(dim, blocks):
        steps = jax.random.uniform(jax.random.fold_in(jax.random.fold_in(rng, 6), dim), (blocks,), jnp.float32, smallest / len(pieces), high / len(pieces))
        return jnp.repeat(jnp.exp(steps), shape[dim] // blocks).reshape((-1,) + (1,) * (len(shape) - dim - 1))

    level = one(*pieces[0])
    for cut in pieces[1:]:
        level = level * one(*cut)
    return level


def bell_draw(key, dims, width, reach, pieces=(), kind=jnp.bfloat16):
    gain = shard_levels(key, dims, pieces, -0.22, 0.18) if pieces else 1.0
    values = jax.random.normal(key, dims, jnp.float32) * width * gain
    return jnp.minimum(jnp.maximum(values, -reach), reach).astype(kind)


def setup_inputs(seed: int = 0) -> dict:
    streams_of = jax.random.split(jax.random.key(seed), 4)
    buffer = draw_buffer(jax.random.fold_in(streams_of[3], 71), 0)
    right_basis = bell_draw(streams_of[1], (LAYER_SLOTS, COLS, RANK), COLS ** -0.5, 0.125, ((0, 4), (1, 8)))
    layer_count = draw_layer_count(jax.random.fold_in(streams_of[3], 71), 0)
    return dict(buffer=buffer, right_basis=right_basis, layer_count=layer_count)


MOMENTUM = 0.9
CLIP_RMS = 0.35
SQUARE_FLOOR = 0.0625

def one_layer(pair):
    block, basis = pair
    proj = jnp.dot(block.astype(jnp.float32), basis.astype(jnp.float32), preferred_element_type=jnp.float32)
    gram = jnp.dot(proj.T, proj, precision=lax.Precision.HIGHEST)
    lower = jnp.linalg.cholesky(gram)
    ortho = jax.scipy.linalg.solve_triangular(lower, proj.T, lower=True).T
    half_left = ortho.astype(jnp.bfloat16)
    right = jnp.dot(block.T.astype(jnp.float32), half_left.astype(jnp.float32), preferred_element_type=jnp.float32)
    half_right = right.astype(jnp.bfloat16)
    correction = jnp.dot(half_left.astype(jnp.float32), half_right.T.astype(jnp.float32), preferred_element_type=jnp.float32)
    moment = (block.astype(jnp.float32) - (1.0 - MOMENTUM) * correction).astype(jnp.bfloat16)
    colsq = lax.optimization_barrier(jnp.sum(right * right, axis=0, keepdims=True))
    scaled = right * (math.sqrt(COLS) * lax.rsqrt(colsq + 1.0))
    squares = jnp.sum(jnp.square(block.astype(jnp.float32)))
    return (moment, ortho, scaled, squares)

def reference(buffer, right_basis, layer_count):
    moment, ortho, scaled, squares = lax.map(one_layer, (buffer, right_basis))
    slot_ids = jnp.arange(LAYER_SLOTS, dtype=jnp.int32)
    used = slot_ids % SLOTS < layer_count[slot_ids // SLOTS]
    total_sq = jnp.sum(jnp.where(used, squares, jnp.float32(0.0)))
    elements = jnp.sum(layer_count).astype(jnp.float32) * jnp.float32(ROWS * COLS)
    clip = jnp.minimum(jnp.float32(1.0), CLIP_RMS * lax.rsqrt(jnp.maximum(total_sq / elements, SQUARE_FLOOR)))
    keep = used[:, None, None]
    momentum_out = jnp.where(keep, moment, jnp.zeros_like(moment))
    left_step = jnp.where(keep, clip * math.sqrt(ROWS) * ortho, jnp.float32(0.0)).astype(jnp.bfloat16)
    right_step = jnp.where(keep, scaled, jnp.float32(0.0))
    return (momentum_out, left_step, right_step)
```

```python
import functools
import math

import jax
import jax.numpy as jnp
from jax import lax
from jax.experimental import pallas as pl
from jax.experimental.pallas import tpu as pltpu
from jax.sharding import PartitionSpec as P

MOMENTUM = 0.9
CLIP_RMS = 0.35
SQUARE_FLOOR = 0.0625
MESH = pl.DeviceIdType.MESH
HIGHEST = lax.Precision.HIGHEST
F32 = jnp.float32
BF16 = jnp.bfloat16
LINK = jnp.float32
VMEM_LIMIT = 60 * 1024 * 1024


def to_index(pos, n):
    if n % 2:
        return pos
    return jnp.where(pos < n // 2, 2 * pos, 2 * (n - 1 - pos) + 1)


def to_pos(index, n):
    if n % 2:
        return index
    return jnp.where(index % 2 == 0, index // 2, n - 1 - index // 2)


def hops_of(slot, way, n):
    return n // 2 if slot % 2 == way else n - 1 - n // 2


def greet(devices):
    barrier = pltpu.get_barrier_semaphore()
    for axis, index in devices:
        pl.semaphore_signal(barrier, inc=1, device_id={axis: index}, device_id_type=MESH)
    pl.semaphore_wait(barrier, len(devices))


def ring(n):
    me = lax.axis_index("shard")
    pos = to_pos(me, n)
    right = to_index((pos + 1) % n, n)
    left = to_index((pos + n - 1) % n, n)
    return me, pos, (right, left)


def ring_gather(n, slots, out_ref, send, recv):
    me, pos, sides = ring(n)
    started = {}
    for hop in range(n // 2 + 1):
        for slot in range(slots):
            for way in range(2):
                total = hops_of(slot, way, n)
                if hop > total:
                    continue
                if hop > 0:
                    started[slot, way, hop - 1].wait_recv()
                if hop == total:
                    continue
                sign = -1 if way == 0 else 1
                owner = to_index((pos + sign * hop + n) % n, n)
                block = out_ref.at[slot, owner]
                copy = pltpu.make_async_remote_copy(
                    src_ref=block,
                    dst_ref=block,
                    send_sem=send.at[slot, way, hop],
                    recv_sem=recv.at[slot, way, hop],
                    device_id={"shard": sides[way]},
                    device_id_type=MESH,
                )
                copy.start()
                started[slot, way, hop] = copy
    for copy in started.values():
        copy.wait_send()


def ring_scatter(n, slots, part_ref, sums, got, send, recv):
    me, pos, sides = ring(n)
    started = {}
    for hop in range(n // 2):
        for slot in range(slots):
            for way in range(2):
                total = hops_of(slot, way, n)
                if hop >= total:
                    continue
                sign = 1 if way == 0 else -1
                owner = to_index((pos + sign * (total - hop) + n) % n, n)
                value = part_ref[slot, owner]
                if hop > 0:
                    started[slot, way, hop - 1].wait_recv()
                    value = value + got[slot, way, hop - 1].astype(F32)
                sums[slot, way, hop] = value.astype(sums.dtype)
                copy = pltpu.make_async_remote_copy(
                    src_ref=sums.at[slot, way, hop],
                    dst_ref=got.at[slot, way, hop],
                    send_sem=send.at[slot, way, hop],
                    recv_sem=recv.at[slot, way, hop],
                    device_id={"shard": sides[way]},
                    device_id_type=MESH,
                )
                copy.start()
                started[slot, way, hop] = copy
    out = []
    for slot in range(slots):
        value = part_ref[slot, me]
        for way in range(2):
            last = hops_of(slot, way, n) - 1
            if last >= 0:
                started[slot, way, last].wait_recv()
                value = value + got[slot, way, last].astype(F32)
        out.append(value)
    for copy in started.values():
        copy.wait_send()
    return out


def exchange(axis, n, source, landing, send, recv):
    me = lax.axis_index(axis)
    copies = []
    for step in range(1, n):
        peer = (me + step) % n
        copy = pltpu.make_async_remote_copy(
            src_ref=source(peer),
            dst_ref=landing.at[me],
            send_sem=send.at[step],
            recv_sem=recv.at[step],
            device_id={axis: peer},
            device_id_type=MESH,
        )
        copy.start()
        copies.append(copy)
    return copies


def others(axis, n):
    me = lax.axis_index(axis)
    return [(axis, (me + step) % n) for step in range(1, n)]


def gather_kernel(n, slots, basis_ref, out_ref, send, recv, local):
    me, _, sides = ring(n)
    copy = pltpu.make_async_copy(basis_ref, out_ref.at[:, me], local)
    copy.start()
    greet([("shard", sides[0]), ("shard", sides[1])])
    copy.wait()
    ring_gather(n, slots, out_ref, send, recv)


def project_kernel(block_ref, basis_ref, proj_ref, gram_ref, part_ref, square_ref):
    block = block_ref[0]
    proj = jnp.dot(block, basis_ref[0], preferred_element_type=F32)
    proj_ref[0] = proj
    gram = lax.dot_general(
        proj, proj, (((0,), (0,)), ((), ())), precision=HIGHEST, preferred_element_type=F32
    )
    part = lax.dot_general(
        block, proj.astype(BF16), (((0,), (0,)), ((), ())), preferred_element_type=F32
    )
    wide = block.astype(F32)
    square = jnp.sum(jnp.square(wide).reshape(-1, 8, wide.shape[1]), axis=0)

    @pl.when(pl.program_id(1) == 0)
    def _():
        gram_ref[0] = gram
        part_ref[0] = part
        square_ref[0] = square

    @pl.when(pl.program_id(1) > 0)
    def _():
        gram_ref[0] += gram
        part_ref[0] += part
        square_ref[0] += square


def reduce_kernel(
    n, segments, slots, gram_ref, stat_ref, part_ref, full_ref, total_ref, own_ref,
    landing, done, stat_in, stat_sum, seg_in, sums, got,
    send_a, recv_a, send_b, recv_b, send_c, recv_c, send_d, recv_d, send_e, recv_e,
):
    me = lax.axis_index("shard")
    seg = lax.axis_index("segment")
    greet(others("shard", n) + others("segment", segments))
    first = exchange("shard", n, lambda peer: gram_ref.at[peer], landing, send_a, recv_a)
    stats = exchange("shard", n, lambda peer: stat_ref, stat_in, send_b, recv_b)
    landing[me] = gram_ref[me]
    stat_in[me] = stat_ref[...]
    for copy in first:
        copy.wait()
    value = landing[0]
    for i in range(1, n):
        value = value + landing[i]
    done[...] = value
    full_ref[me] = value
    second = exchange("shard", n, lambda peer: done, full_ref, send_c, recv_c)
    for copy in stats:
        copy.wait()
    value = stat_in[0]
    for i in range(1, n):
        value = value + stat_in[i]
    stat_sum[...] = value
    seg_in[seg] = value
    last = exchange("segment", segments, lambda peer: stat_sum, seg_in, send_d, recv_d)
    own = ring_scatter(n, slots, part_ref, sums, got, send_e, recv_e)
    for slot in range(slots):
        own_ref[slot] = own[slot]
    for copy in last + second:
        copy.wait()
    value = seg_in[0]
    for i in range(1, segments):
        value = value + seg_in[i]
    total_ref[...] = value


def eliminate(blocks):
    size = blocks[0].shape[0]
    rows = lax.broadcasted_iota(jnp.int32, (size, size), 0)
    lanes = lax.broadcasted_iota(jnp.int32, (size, size), 1)

    def step(j, blocks):
        out = []
        for m in blocks:
            row = jnp.sum(jnp.where(rows == j, m, 0.0), axis=0, keepdims=True)
            col = jnp.sum(jnp.where(lanes == j, m, 0.0), axis=1, keepdims=True)
            lane = lanes[:1] == j
            pivot = jnp.sum(jnp.where(lane, row, 0.0), axis=1, keepdims=True)
            scaled = jnp.where(lane, 1.0, row) / pivot
            below = rows > j
            kept = jnp.where(below & (lanes == j), 0.0, m)
            out.append(kept - jnp.where(below, col, 0.0) * scaled)
        return tuple(out)

    blocks = lax.fori_loop(0, size, step, tuple(blocks))
    result = []
    for m in blocks:
        diag = jnp.sum(jnp.where(lanes == rows, m, 0.0), axis=1, keepdims=True)
        unit = jnp.where(lanes < rows, m, jnp.where(lanes == rows, 1.0, 0.0))
        result.append(unit * lax.rsqrt(diag))
    return result


def mm(a, b, dims):
    return lax.dot_general(a, b, ((dims[:1], dims[1:]), ((), ())), precision=HIGHEST, preferred_element_type=F32)


def factor_kernel(slots, gram_ref, inv_ref):
    half = gram_ref.shape[1] // 2
    heads = eliminate([gram_ref[s, :half, :half] for s in range(slots)])
    sides = [mm(gram_ref[s, half:, :half], heads[s], (1, 1)) for s in range(slots)]
    rests = [gram_ref[s, half:, half:] - mm(sides[s], sides[s], (1, 1)) for s in range(slots)]
    tails = eliminate(rests)
    for s in range(slots):
        inv_ref[s, :half, :half] = heads[s]
        inv_ref[s, :half, half:] = jnp.zeros((half, half), F32)
        inv_ref[s, half:, :half] = -mm(tails[s], mm(sides[s], heads[s], (1, 0)), (1, 0))
        inv_ref[s, half:, half:] = tails[s]


def right_kernel(
    n, slots, cols, own_ref, inv_ref, right_ref, full_ref, mine, sq_in, send_a, recv_a, send_b, recv_b
):
    me, _, sides = ring(n)
    greet(others("shard", n))
    values = []
    mine[...] = jnp.zeros_like(mine)
    for slot in range(slots):
        value = mm(own_ref[slot], inv_ref[slot], (1, 1))
        full_ref[slot, me] = value.astype(BF16)
        mine[slot : slot + 1] = jnp.sum(value * value, axis=0, keepdims=True)
        right_ref[slot] = value
    copies = exchange("shard", n, lambda peer: mine, sq_in, send_a, recv_a)
    sq_in[me] = mine[...]
    ring_gather(n, slots, full_ref, send_b, recv_b)
    for copy in copies:
        copy.wait()
    total = sq_in[0]
    for i in range(1, n):
        total = total + sq_in[i]
    scale = math.sqrt(cols) * lax.rsqrt(total + 1.0)
    for slot in range(slots):
        right_ref[slot] = right_ref[slot] * scale[slot : slot + 1]


def final_kernel(scale_ref, count_ref, block_ref, proj_ref, inv_ref, basis_ref, moment_ref, left_ref):
    keep = pl.program_id(0) < count_ref[0]

    @pl.when(keep)
    def _():
        ortho = mm(proj_ref[0], inv_ref[0], (1, 1))
        half = ortho.astype(BF16)
        fix = lax.dot_general(half, basis_ref[0], (((1,), (1,)), ((), ())), preferred_element_type=F32)
        moment_ref[0] = (block_ref[0].astype(F32) - (1.0 - MOMENTUM) * fix).astype(BF16)
        left_ref[0] = (scale_ref[0] * ortho).astype(BF16)

    @pl.when(jnp.logical_not(keep))
    def _():
        moment_ref[...] = jnp.zeros_like(moment_ref)
        left_ref[...] = jnp.zeros_like(left_ref)


def vmem():
    return pl.BlockSpec(memory_space=pltpu.VMEM)


def comm(collective_id):
    return pltpu.CompilerParams(
        collective_id=collective_id, has_side_effects=True, vmem_limit_bytes=VMEM_LIMIT
    )


def body(buffer, right_basis, layer_count):
    n = lax.axis_size("shard")
    segments = lax.axis_size("segment")
    slots, rows_dev, cols = buffer.shape
    width, rank = right_basis.shape[1:]
    rows_all = rows_dev * n
    dma = pltpu.SemaphoreType.DMA
    hops = max(n // 2, 1)
    shape = jax.ShapeDtypeStruct
    count = layer_count[0]

    basis = pl.pallas_call(
        functools.partial(gather_kernel, n, slots),
        out_shape=shape((slots, n, width, rank), BF16),
        in_specs=[vmem()],
        out_specs=vmem(),
        scratch_shapes=[dma((slots, 2, hops)), dma((slots, 2, hops)), dma],
        compiler_params=comm(0),
        name="gather_basis",
    )(right_basis).reshape(slots, cols, rank)

    tile = math.gcd(rows_dev, 256)
    tiles = rows_dev // tile
    per_tile = pl.BlockSpec((1, tile, cols), lambda s, i: (s, i, 0))
    proj_tile = pl.BlockSpec((1, tile, rank), lambda s, i: (s, i, 0))

    def per_slot(*dims):
        return pl.BlockSpec((1,) + dims, lambda s, i: (s, 0, 0))

    proj, gram, part, square = pl.pallas_call(
        project_kernel,
        grid=(slots, tiles),
        out_shape=(
            shape((slots, rows_dev, rank), F32),
            shape((slots, rank, rank), F32),
            shape((slots, cols, rank), F32),
            shape((slots, 8, cols), F32),
        ),
        in_specs=[per_tile, per_slot(cols, rank)],
        out_specs=(proj_tile, per_slot(rank, rank), per_slot(cols, rank), per_slot(8, cols)),
        compiler_params=pltpu.CompilerParams(vmem_limit_bytes=VMEM_LIMIT),
        name="project",
    )(buffer, basis)

    used = jnp.arange(slots, dtype=jnp.int32) < count
    local_sq = jnp.sum(jnp.where(used, jnp.sum(square, axis=(1, 2)), 0.0))
    local_elems = count.astype(F32) * float(rows_dev * cols)
    odd = lax.broadcasted_iota(jnp.int32, (8, 128), 0) % 2 == 1
    stat = jnp.where(odd, local_elems, local_sq)
    chunk = slots * rank // n

    full_gram, total, own = pl.pallas_call(
        functools.partial(reduce_kernel, n, segments, slots),
        out_shape=(
            shape((n, chunk, rank), F32),
            shape((8, 128), F32),
            shape((slots, width, rank), F32),
        ),
        in_specs=[vmem()] * 3,
        out_specs=(vmem(),) * 3,
        scratch_shapes=[
            pltpu.VMEM((n, chunk, rank), F32),
            pltpu.VMEM((chunk, rank), F32),
            pltpu.VMEM((n, 8, 128), F32),
            pltpu.VMEM((8, 128), F32),
            pltpu.VMEM((segments, 8, 128), F32),
            pltpu.VMEM((slots, 2, hops, width, rank), LINK),
            pltpu.VMEM((slots, 2, hops, width, rank), LINK),
            dma((n,)), dma((n,)), dma((n,)), dma((n,)), dma((n,)), dma((n,)),
            dma((segments,)), dma((segments,)),
            dma((slots, 2, hops)), dma((slots, 2, hops)),
        ],
        compiler_params=comm(1),
        name="reduce",
    )(gram.reshape(n, chunk, rank), stat, part.reshape(slots, n, width, rank))

    inverse = pl.pallas_call(
        functools.partial(factor_kernel, slots),
        out_shape=shape((slots, rank, rank), F32),
        in_specs=[vmem()],
        out_specs=vmem(),
        name="factor",
    )(full_gram.reshape(slots, rank, rank))

    right, half_right = pl.pallas_call(
        functools.partial(right_kernel, n, slots, cols),
        out_shape=(shape((slots, width, rank), F32), shape((slots, n, width, rank), BF16)),
        in_specs=[vmem()] * 2,
        out_specs=(vmem(),) * 2,
        scratch_shapes=[
            pltpu.VMEM((8, rank), F32),
            pltpu.VMEM((n, 8, rank), F32),
            dma((n,)), dma((n,)),
            dma((slots, 2, hops)), dma((slots, 2, hops)),
        ],
        compiler_params=comm(2),
        name="right",
    )(own, inverse)

    clip = jnp.minimum(1.0, CLIP_RMS * lax.rsqrt(jnp.maximum(total[0, 0] / total[1, 0], SQUARE_FLOOR)))
    scale = (clip * math.sqrt(rows_all)).reshape(1)
    smem = pl.BlockSpec(memory_space=pltpu.SMEM)
    moment, left = pl.pallas_call(
        final_kernel,
        grid=(slots, tiles),
        out_shape=(shape(buffer.shape, BF16), shape((slots, rows_dev, rank), BF16)),
        in_specs=[smem, smem, per_tile, proj_tile, per_slot(rank, rank), per_slot(cols, rank)],
        out_specs=(per_tile, proj_tile),
        compiler_params=pltpu.CompilerParams(vmem_limit_bytes=VMEM_LIMIT),
        name="final",
    )(scale, layer_count, buffer, proj, inverse, half_right.reshape(slots, cols, rank))
    return (moment, left, jnp.where(used[:, None, None], right, 0.0))


def solution(mesh):
    in_specs = (P("segment", "shard", None), P("segment", "shard", None), P("segment"))
    out_specs = (
        P("segment", "shard", None),
        P("segment", "shard", None),
        P("segment", "shard", None),
    )
    return jax.shard_map(body, mesh=mesh, in_specs=in_specs, out_specs=out_specs, check_vma=False)
```

```python
import functools
import math

import jax
import jax.numpy as jnp
from jax import lax
from jax.experimental import pallas as pl
from jax.experimental.pallas import tpu as pltpu
from jax.sharding import PartitionSpec as P

MOMENTUM = 0.9
CLIP_RMS = 0.35
SQUARE_FLOOR = 0.0625
MESH = pl.DeviceIdType.MESH
HIGHEST = lax.Precision.HIGHEST
F32 = jnp.float32
BF16 = jnp.bfloat16
LINK = jnp.float32
VMEM_LIMIT = 60 * 1024 * 1024


def to_index(pos, n):
    if n % 2:
        return pos
    return jnp.where(pos < n // 2, 2 * pos, 2 * (n - 1 - pos) + 1)


def to_pos(index, n):
    if n % 2:
        return index
    return jnp.where(index % 2 == 0, index // 2, n - 1 - index // 2)


def hops_of(slot, way, n):
    return n // 2 if slot % 2 == way else n - 1 - n // 2


def greet(devices):
    barrier = pltpu.get_barrier_semaphore()
    for axis, index in devices:
        pl.semaphore_signal(barrier, inc=1, device_id={axis: index}, device_id_type=MESH)
    pl.semaphore_wait(barrier, len(devices))


def ring(n):
    me = lax.axis_index("shard")
    pos = to_pos(me, n)
    right = to_index((pos + 1) % n, n)
    left = to_index((pos + n - 1) % n, n)
    return me, pos, (right, left)


def ring_gather(n, slots, out_ref, send, recv):
    me, pos, sides = ring(n)
    started = {}
    for hop in range(n // 2 + 1):
        for slot in range(slots):
            for way in range(2):
                total = hops_of(slot, way, n)
                if hop > total:
                    continue
                if hop > 0:
                    started[slot, way, hop - 1].wait_recv()
                if hop == total:
                    continue
                sign = -1 if way == 0 else 1
                owner = to_index((pos + sign * hop + n) % n, n)
                block = out_ref.at[slot, owner]
                copy = pltpu.make_async_remote_copy(
                    src_ref=block,
                    dst_ref=block,
                    send_sem=send.at[slot, way, hop],
                    recv_sem=recv.at[slot, way, hop],
                    device_id={"shard": sides[way]},
                    device_id_type=MESH,
                )
                copy.start()
                started[slot, way, hop] = copy
    for copy in started.values():
        copy.wait_send()


def ring_scatter(n, slots, part_ref, sums, got, send, recv, between):
    me, pos, sides = ring(n)
    started = {}
    for hop in range(n // 2):
        for slot in range(slots):
            for way in range(2):
                total = hops_of(slot, way, n)
                if hop >= total:
                    continue
                sign = 1 if way == 0 else -1
                owner = to_index((pos + sign * (total - hop) + n) % n, n)
                value = part_ref[slot, owner]
                if hop > 0:
                    started[slot, way, hop - 1].wait_recv()
                    value = value + got[slot, way, hop - 1].astype(F32)
                sums[slot, way, hop] = value.astype(sums.dtype)
                copy = pltpu.make_async_remote_copy(
                    src_ref=sums.at[slot, way, hop],
                    dst_ref=got.at[slot, way, hop],
                    send_sem=send.at[slot, way, hop],
                    recv_sem=recv.at[slot, way, hop],
                    device_id={"shard": sides[way]},
                    device_id_type=MESH,
                )
                copy.start()
                started[slot, way, hop] = copy
        between(hop)
    out = []
    for slot in range(slots):
        value = part_ref[slot, me]
        for way in range(2):
            last = hops_of(slot, way, n) - 1
            if last >= 0:
                started[slot, way, last].wait_recv()
                value = value + got[slot, way, last].astype(F32)
        out.append(value)
    for copy in started.values():
        copy.wait_send()
    return out


def exchange(axis, n, source, landing, send, recv):
    me = lax.axis_index(axis)
    copies = []
    for step in range(1, n):
        peer = (me + step) % n
        copy = pltpu.make_async_remote_copy(
            src_ref=source(peer),
            dst_ref=landing.at[me],
            send_sem=send.at[step],
            recv_sem=recv.at[step],
            device_id={axis: peer},
            device_id_type=MESH,
        )
        copy.start()
        copies.append(copy)
    return copies


def others(axis, n):
    me = lax.axis_index(axis)
    return [(axis, (me + step) % n) for step in range(1, n)]


def gather_kernel(n, slots, basis_ref, out_ref, send, recv, local):
    me, _, sides = ring(n)
    copy = pltpu.make_async_copy(basis_ref, out_ref.at[:, me], local)
    copy.start()
    greet([("shard", sides[0]), ("shard", sides[1])])
    copy.wait()
    ring_gather(n, slots, out_ref, send, recv)


def split(value):
    high = value.astype(BF16)
    return high, (value - high.astype(F32)).astype(BF16)


def dot(a, b, dims):
    return lax.dot_general(a, b, ((dims[:1], dims[1:]), ((), ())), preferred_element_type=F32)


def project_kernel(block_ref, basis_ref, proj_ref, gram_ref, part_ref, square_ref, cross):
    block = block_ref[0]
    proj = jnp.dot(block, basis_ref[0], preferred_element_type=F32)
    proj_ref[0] = proj
    high, low = split(proj)
    gram = dot(high, high, (0, 0)) + dot(low, low, (0, 0))
    mixed = dot(high, low, (0, 0))
    part = dot(block, high, (0, 0))
    wide = block.astype(F32)
    square = jnp.sum(jnp.square(wide).reshape(-1, 8, wide.shape[1]), axis=0)
    half = gram.shape[0] // 2

    @pl.when(pl.program_id(1) == 0)
    def _():
        cross[0] = gram
        cross[1] = mixed
        part_ref[0] = part
        square_ref[0] = square

    @pl.when(pl.program_id(1) > 0)
    def _():
        cross[0] += gram
        cross[1] += mixed
        part_ref[0] += part
        square_ref[0] += square

    @pl.when(pl.program_id(1) == pl.num_programs(1) - 1)
    def _():
        whole = cross[0] + cross[1] + cross[1].T
        gram_ref[0, 0] = whole[:half, :half]
        gram_ref[0, 1] = whole[half:, :half]
        gram_ref[0, 2] = whole[half:, half:]


def mm(a, b, dims):
    return lax.dot_general(a, b, ((dims[:1], dims[1:]), ((), ())), precision=HIGHEST, preferred_element_type=F32)


def eliminate(blocks, first, last):
    size = blocks[0].shape[0]
    rows = lax.broadcasted_iota(jnp.int32, (size, size), 0)
    lanes = lax.broadcasted_iota(jnp.int32, (size, size), 1)

    def step(j, blocks):
        out = []
        for m in blocks:
            row = jnp.sum(jnp.where(rows == j, m, 0.0), axis=0, keepdims=True)
            col = jnp.sum(jnp.where(lanes == j, m, 0.0), axis=1, keepdims=True)
            lane = lanes[:1] == j
            pivot = jnp.sum(jnp.where(lane, row, 0.0), axis=1, keepdims=True)
            scaled = jnp.where(lane, 1.0, row) / pivot
            below = rows > j
            kept = jnp.where(below & (lanes == j), 0.0, m)
            out.append(kept - jnp.where(below, col, 0.0) * scaled)
        return tuple(out)

    return lax.fori_loop(first, last, step, tuple(blocks))


def inverse_of(m):
    rows = lax.broadcasted_iota(jnp.int32, m.shape, 0)
    lanes = lax.broadcasted_iota(jnp.int32, m.shape, 1)
    diag = jnp.sum(jnp.where(lanes == rows, m, 0.0), axis=1, keepdims=True)
    unit = jnp.where(lanes < rows, m, jnp.where(lanes == rows, 1.0, 0.0))
    return unit * lax.rsqrt(diag)


def factor_pieces(slots, full_ref, work, side, inv_ref):
    half = work.shape[1]

    def run(first, last):
        done = eliminate([work[s] for s in range(slots)], first, last)
        for s in range(slots):
            work[s] = done[s]

    def start():
        grams = full_ref[...].reshape(slots, 3, half, half)
        for s in range(slots):
            work[s] = grams[s, 0]
        run(0, half // 2)

    def turn():
        run(half // 2, half)
        grams = full_ref[...].reshape(slots, 3, half, half)
        for s in range(slots):
            head = inverse_of(work[s])
            edge = mm(grams[s, 1], head, (1, 1))
            inv_ref[s, :half, :half] = head
            inv_ref[s, :half, half:] = jnp.zeros((half, half), F32)
            side[s] = mm(edge, head, (1, 0))
            work[s] = grams[s, 2] - mm(edge, edge, (1, 1))

    def middle():
        run(0, half // 2)

    def end():
        run(half // 2, half)
        for s in range(slots):
            tail = inverse_of(work[s])
            inv_ref[s, half:, :half] = -mm(tail, side[s], (1, 0))
            inv_ref[s, half:, half:] = tail

    return [start, turn, middle, end]


def add_up(ref, count):
    value = ref[0]
    for i in range(1, count):
        value = value + ref[i]
    return value


def reduce_kernel(
    n, segments, slots, cols, gram_ref, stat_ref, part_ref, total_ref, inv_ref, right_ref, basis_ref,
    full, landing, done, stat_in, stat_sum, seg_in, sums, got, work, side, mine, sq_in,
    send_a, recv_a, send_b, recv_b, send_c, recv_c, send_d, recv_d, send_e, recv_e,
    send_f, recv_f, send_g, recv_g,
):
    me = lax.axis_index("shard")
    seg = lax.axis_index("segment")
    greet(others("shard", n) + others("segment", segments))
    first = exchange("shard", n, lambda peer: gram_ref.at[peer], landing, send_a, recv_a)
    stats = exchange("shard", n, lambda peer: stat_ref, stat_in, send_b, recv_b)
    landing[me] = gram_ref[me]
    stat_in[me] = stat_ref[...]
    for copy in first:
        copy.wait()
    value = add_up(landing, n)
    done[...] = value
    full[me] = value
    second = exchange("shard", n, lambda peer: done, full, send_c, recv_c)
    for copy in stats:
        copy.wait()
    value = add_up(stat_in, n)
    stat_sum[...] = value
    seg_in[seg] = value
    third = exchange("segment", segments, lambda peer: stat_sum, seg_in, send_d, recv_d)
    pieces = factor_pieces(slots, full, work, side, inv_ref)
    hops = n // 2

    def between(hop):
        if hop == 0:
            for copy in second:
                copy.wait()
        for i, piece in enumerate(pieces):
            if i * hops // len(pieces) == hop:
                piece()

    own = ring_scatter(n, slots, part_ref, sums, got, send_e, recv_e, between)
    mine[...] = jnp.zeros_like(mine)
    for slot in range(slots):
        value = mm(own[slot], inv_ref[slot], (1, 1))
        basis_ref[slot, me] = value.astype(BF16)
        mine[slot : slot + 1] = jnp.sum(value * value, axis=0, keepdims=True)
        right_ref[slot] = value
    squares = exchange("shard", n, lambda peer: mine, sq_in, send_f, recv_f)
    sq_in[me] = mine[...]
    ring_gather(n, slots, basis_ref, send_g, recv_g)
    for copy in squares + third:
        copy.wait()
    total_ref[...] = add_up(seg_in, segments)
    scale = math.sqrt(cols) * lax.rsqrt(add_up(sq_in, n) + 1.0)
    for slot in range(slots):
        right_ref[slot] = right_ref[slot] * scale[slot : slot + 1]


def final_kernel(scale_ref, count_ref, block_ref, proj_ref, inv_ref, basis_ref, moment_ref, left_ref):
    keep = pl.program_id(0) < count_ref[0]

    @pl.when(keep)
    def _():
        high, low = split(proj_ref[0])
        top, rest = split(inv_ref[0])
        ortho = dot(high, top, (1, 1)) + (dot(high, rest, (1, 1)) + dot(low, top, (1, 1)))
        fix = dot(ortho.astype(BF16), basis_ref[0], (1, 1))
        moment_ref[0] = (block_ref[0].astype(F32) - (1.0 - MOMENTUM) * fix).astype(BF16)
        left_ref[0] = (scale_ref[0] * ortho).astype(BF16)

    @pl.when(jnp.logical_not(keep))
    def _():
        moment_ref[...] = jnp.zeros_like(moment_ref)
        left_ref[...] = jnp.zeros_like(left_ref)


def vmem():
    return pl.BlockSpec(memory_space=pltpu.VMEM)


def comm(collective_id):
    return pltpu.CompilerParams(
        collective_id=collective_id, has_side_effects=True, vmem_limit_bytes=VMEM_LIMIT
    )


def body(buffer, right_basis, layer_count):
    n = lax.axis_size("shard")
    segments = lax.axis_size("segment")
    slots, rows_dev, cols = buffer.shape
    width, rank = right_basis.shape[1:]
    rows_all = rows_dev * n
    dma = pltpu.SemaphoreType.DMA
    hops = max(n // 2, 1)
    shape = jax.ShapeDtypeStruct
    count = layer_count[0]

    basis = pl.pallas_call(
        functools.partial(gather_kernel, n, slots),
        out_shape=shape((slots, n, width, rank), BF16),
        in_specs=[vmem()],
        out_specs=vmem(),
        scratch_shapes=[dma((slots, 2, hops)), dma((slots, 2, hops)), dma],
        compiler_params=comm(0),
        name="gather_basis",
    )(right_basis).reshape(slots, cols, rank)

    half = rank // 2
    tile = math.gcd(rows_dev, 768)
    tiles = rows_dev // tile
    per_tile = pl.BlockSpec((1, tile, cols), lambda s, i: (s, i, 0))
    proj_tile = pl.BlockSpec((1, tile, rank), lambda s, i: (s, i, 0))

    def per_slot(*dims):
        return pl.BlockSpec((1,) + dims, lambda s, i: (s, 0, 0))

    proj, gram, part, square = pl.pallas_call(
        project_kernel,
        grid=(slots, tiles),
        out_shape=(
            shape((slots, rows_dev, rank), F32),
            shape((slots, 3, half, half), F32),
            shape((slots, cols, rank), F32),
            shape((slots, 8, cols), F32),
        ),
        in_specs=[per_tile, per_slot(cols, rank)],
        out_specs=(
            proj_tile,
            pl.BlockSpec((1, 3, half, half), lambda s, i: (s, 0, 0, 0)),
            per_slot(cols, rank),
            per_slot(8, cols),
        ),
        scratch_shapes=[pltpu.VMEM((2, rank, rank), F32)],
        compiler_params=pltpu.CompilerParams(vmem_limit_bytes=VMEM_LIMIT),
        name="project",
    )(buffer, basis)

    used = jnp.arange(slots, dtype=jnp.int32) < count
    local_sq = jnp.sum(jnp.where(used, jnp.sum(square, axis=(1, 2)), 0.0))
    local_elems = count.astype(F32) * float(rows_dev * cols)
    odd = lax.broadcasted_iota(jnp.int32, (8, 128), 0) % 2 == 1
    stat = jnp.where(odd, local_elems, local_sq)
    chunk = slots * 3 * half // n

    total, inverse, right, half_right = pl.pallas_call(
        functools.partial(reduce_kernel, n, segments, slots, cols),
        out_shape=(
            shape((8, 128), F32),
            shape((slots, rank, rank), F32),
            shape((slots, width, rank), F32),
            shape((slots, n, width, rank), BF16),
        ),
        in_specs=[vmem()] * 3,
        out_specs=(vmem(),) * 4,
        scratch_shapes=[
            pltpu.VMEM((n, chunk, half), F32),
            pltpu.VMEM((n, chunk, half), F32),
            pltpu.VMEM((chunk, half), F32),
            pltpu.VMEM((n, 8, 128), F32),
            pltpu.VMEM((8, 128), F32),
            pltpu.VMEM((segments, 8, 128), F32),
            pltpu.VMEM((slots, 2, hops, width, rank), LINK),
            pltpu.VMEM((slots, 2, hops, width, rank), LINK),
            pltpu.VMEM((slots, half, half), F32),
            pltpu.VMEM((slots, half, half), F32),
            pltpu.VMEM((8, rank), F32),
            pltpu.VMEM((n, 8, rank), F32),
            dma((n,)), dma((n,)), dma((n,)), dma((n,)), dma((n,)), dma((n,)),
            dma((segments,)), dma((segments,)),
            dma((slots, 2, hops)), dma((slots, 2, hops)),
            dma((n,)), dma((n,)),
            dma((slots, 2, hops)), dma((slots, 2, hops)),
        ],
        compiler_params=comm(1),
        name="reduce",
    )(gram.reshape(n, chunk, half), stat, part.reshape(slots, n, width, rank))

    clip = jnp.minimum(1.0, CLIP_RMS * lax.rsqrt(jnp.maximum(total[0, 0] / total[1, 0], SQUARE_FLOOR)))
    scale = (clip * math.sqrt(rows_all)).reshape(1)
    smem = pl.BlockSpec(memory_space=pltpu.SMEM)
    moment, left = pl.pallas_call(
        final_kernel,
        grid=(slots, tiles),
        out_shape=(shape(buffer.shape, BF16), shape((slots, rows_dev, rank), BF16)),
        in_specs=[smem, smem, per_tile, proj_tile, per_slot(rank, rank), per_slot(cols, rank)],
        out_specs=(per_tile, proj_tile),
        compiler_params=pltpu.CompilerParams(vmem_limit_bytes=VMEM_LIMIT),
        name="final",
    )(scale, layer_count, buffer, proj, inverse, half_right.reshape(slots, cols, rank))
    return (moment, left, jnp.where(used[:, None, None], right, 0.0))


def solution(mesh):
    in_specs = (P("segment", "shard", None), P("segment", "shard", None), P("segment"))
    out_specs = (
        P("segment", "shard", None),
        P("segment", "shard", None),
        P("segment", "shard", None),
    )
    return jax.shard_map(body, mesh=mesh, in_specs=in_specs, out_specs=out_specs, check_vma=False)
```
